256 devices in a mesh: task: 32 (over z, y), occ: 8 (over x, core).
Axes of the slice: x: 4, y: 4, z: 8, core: 2. Of those that a mesh axis runs over, the one named last changes fastest.
Arguments:
- ao_tiles: bfloat16 [5120, 8, 32, 128], P('task'), may hold values from -6 to 6
- mo_coeffs: bfloat16 [1536, 200], P(None, 'occ'), may hold values from -0.5 to 0.5
- mu_blocks: int32 [5120], P('task'), may hold values from 0 to 191
- nu_blocks: int32 [5120], P('task'), may hold values from 0 to 47
- tile_live: int32 [5120], P('task'), may hold values 0 or 1
- batch_target: int32 [640], P('task'), may hold values from 0 to 2
- batch_count: int32 [32], P('task'), may hold values from 1 to 20
Outputs:
- half_mo: float32 [200, 200, 4096], P('occ', None, 'task')
The draws below stay inside these ranges and needn't reach their ends.
Inputs may be any that keep to these rules, and one draw needn't show every extreme that they name: `batch_target`: the batch's kl block is the block owned by task index (own index + value) mod 32. `batch_count`: batches at or after this count in a list are not part of the work.
All inputs are finite; a program needn't handle non-finite values. No bound on the sum of `tile_live` on one device may be relied on, other than what follows from the above.
Results may differ from the reference program's by a relative error of at most 0.0029.
Values may be sent and summed in bfloat16 or wider, within the bound.
No kernel may reach another device: no remote copies, remote signals or barrier semaphores. Data moves between devices by JAX's collectives and lax.ppermute only.
A program may use at most 128 MiB of HBM per device.

```python
import jax
import jax.numpy as jnp
from jax import lax

NBF = 1536
NOCC = 200
MUT = 8
NUT = 32
KLW = 128
BATCH = 8
NB = 20
SPREAD = 3
BLOCKS = 640
TILES = 5120
N_TASK = 32


def with_ends(result, rng, smallest, largest):
    index_at = [jax.random.randint(jax.random.fold_in(rng, axis), (), 0, length) for axis, length in enumerate(result.shape)]
    widest = result.shape.index(max(result.shape))
    neighbour = index_at[:widest] + [(index_at[widest] + 1) % result.shape[widest]] + index_at[widest + 1:]
    return result.at[tuple(index_at)].set(smallest).at[tuple(neighbour)].set(largest)


def steps_of(own_key, shape, cuts, least, high):
    gain, own = 1.0, jax.random.fold_in(own_key, 6)
    for dim, shards_of in cuts:
        heights = jnp.exp(jax.random.uniform(jax.random.fold_in(own, dim), (shards_of,), jnp.float32, least / len(cuts), high / len(cuts)))
        gain = gain * jnp.repeat(heights, shape[dim] // shards_of).reshape([-1 if axis == dim else 1 for axis in range(len(shape))])
    return gain


def scatter_about(own_key, dims, spread, reach, split=(), held_as=jnp.bfloat16):
    level = steps_of(own_key, dims, split, -0.22, 0.18) if split else 1.0
    array = jax.random.normal(own_key, dims, jnp.float32) * spread * level
    return jnp.minimum(jnp.maximum(array, -reach), reach).astype(held_as)


def setup_inputs(seed: int = 0) -> dict:
    key_list = jax.random.split(jax.random.key(seed), 8)
    return {
        "ao_tiles": scatter_about(key_list[0], (TILES, MUT, NUT, KLW), 1.0, 6.0, ((0, 32),)),
        "mo_coeffs": scatter_about(key_list[1], (NBF, NOCC), 128 ** -0.5, 0.5, ((1, 8),)),
        "mu_blocks": with_ends(jax.random.randint(key_list[2], (TILES,), 0, NBF // MUT), jax.random.fold_in(key_list[2], 1), 0, (NBF // MUT) - 1).astype(jnp.int32),
        "nu_blocks": with_ends(jax.random.randint(key_list[3], (TILES,), 0, NBF // NUT), jax.random.fold_in(key_list[3], 1), 0, (NBF // NUT) - 1).astype(jnp.int32),
        "tile_live": with_ends((jax.random.randint(key_list[4], (TILES,), 0, 4) < 3).astype(jnp.int32), jax.random.fold_in(key_list[4], 1), 0, 1),
        "batch_target": with_ends(jax.random.randint(key_list[5], (BLOCKS,), 0, SPREAD), jax.random.fold_in(key_list[5], 1), 0, SPREAD - 1).astype(jnp.int32),
        "batch_count": with_ends(jax.random.randint(key_list[6], (N_TASK,), 1, NB + 1), jax.random.fold_in(key_list[6], 1), 1, NB).astype(jnp.int32),
    }


def reference(ao_tiles, mo_coeffs, mu_blocks, nu_blocks, tile_live, batch_target, batch_count):
    coeff_full = mo_coeffs.astype(jnp.float32)
    tiles_all = ao_tiles.reshape(N_TASK, NB, BATCH, MUT, NUT, KLW)
    mu_all = mu_blocks.reshape(N_TASK, NB, BATCH)
    nu_all = nu_blocks.reshape(N_TASK, NB, BATCH)
    live_all = tile_live.reshape(N_TASK, NB, BATCH)
    target_all = batch_target.reshape(N_TASK, NB)
    mu_offsets = jnp.arange(MUT, dtype=jnp.int32)
    nu_offsets = jnp.arange(NUT, dtype=jnp.int32)
    spread_ids = jnp.arange(SPREAD, dtype=jnp.int32)

    def one_group(output, group_items):
        tiles_g, mu_g, nu_g, live_g, target_g, listed, group_index = group_items

        def one_batch(partials, batch_items):
            tile_block, mu_ids, nu_ids, live_ids, target, batch_index = batch_items
            coeff_mu = coeff_full[mu_ids[:, None] * MUT + mu_offsets[None, :]]
            quarter = jnp.einsum("bmi,bmnk->bink", coeff_mu, tile_block.astype(jnp.float32)).astype(jnp.bfloat16)
            kept_tiles = (live_ids * (batch_index < listed).astype(jnp.int32)).astype(jnp.float32)
            coeff_nu = coeff_full[nu_ids[:, None] * NUT + nu_offsets[None, :]] * kept_tiles[:, None, None]
            contribution = jnp.einsum("bnj,bink->ijk", coeff_nu, quarter.astype(jnp.float32))
            chosen = (spread_ids == target).astype(jnp.float32)
            return partials + chosen[:, None, None, None] * contribution[None], None

        initial = jnp.zeros((SPREAD, NOCC, NOCC, KLW), jnp.float32)
        partials = lax.scan(one_batch, initial, (tiles_g, mu_g, nu_g, live_g, target_g, jnp.arange(NB, dtype=jnp.int32)))[0]
        for spread_index in range(SPREAD):
            owner_index = (group_index + spread_index) % N_TASK
            column = (owner_index * KLW).astype(jnp.int32)
            earlier = lax.dynamic_slice_in_dim(output, column, KLW, 2)
            output = lax.dynamic_update_slice_in_dim(output, earlier + partials[spread_index], column, 2)
        return output, None

    output = jnp.zeros((NOCC, NOCC, N_TASK * KLW), jnp.float32)
    output = lax.scan(one_group, output, (tiles_all, mu_all, nu_all, live_all, target_all, batch_count, jnp.arange(N_TASK, dtype=jnp.int32)))[0]
    return output
```

```python
import functools

import jax
import jax.numpy as jnp
from jax import lax
from jax.experimental import pallas as pl
from jax.experimental.pallas import tpu as pltpu
from jax.sharding import PartitionSpec as P

SPREAD = 3
GROUP = 8
BUFFERS = 4


def prep_kernel(mu_ref, nu_ref, live_ref, target_ref, count_ref, coeff_ref, slot_out, mu_out, nu_out, n_out, expand_ref, *, stride, zero_block, per_batch):
    for s in range(SPREAD):
        n_out[s] = 0

    def one_batch(b, carry):
        s = target_ref[b]
        base = s * stride
        n = n_out[s]
        for q in range(per_batch):
            g = b * per_batch + q
            slot_out[base + n] = g
            mu_out[base + n] = mu_ref[g]
            nu_out[base + n] = nu_ref[g]
            n = n + live_ref[g]
        n_out[s] = n
        return carry

    lax.fori_loop(0, count_ref[0], one_batch, 0)
    for s in range(SPREAD):
        n = n_out[s]
        for q in range(GROUP):
            slot_out[s * stride + n + q] = 0
            mu_out[s * stride + n + q] = 0
            nu_out[s * stride + n + q] = zero_block
    rows = lax.broadcasted_iota(jnp.int32, (128, 128), 0)
    lanes = lax.broadcasted_iota(jnp.int32, (128, 128), 1)
    chunks = coeff_ref.shape[1] // 128
    for part in range(16):
        select = jnp.where(rows == part * 8 + lanes // 16, 1.0, 0.0).astype(jnp.bfloat16)
        for chunk in range(chunks):
            expand_ref[chunk * 16 + part, : coeff_ref.shape[0], :] = jnp.dot(
                coeff_ref[:, chunk * 128 : (chunk + 1) * 128], select, preferred_element_type=jnp.float32
            )


def partial_kernel(slot_ref, mu_ref, nu_ref, n_ref, tiles_ref, expand_ref, coeff_ref, out_ref, tile_buf, quarter, acc, sems, *, target, stride):
    occ, all_occ, kl = out_ref.shape
    base = target * stride
    groups = (n_ref[target] + GROUP - 1) // GROUP

    def copy(c, buf, q):
        slot = slot_ref[base + c * GROUP + q]
        return pltpu.make_async_copy(tiles_ref.at[slot], tile_buf.at[buf, q], sems.at[buf, q])

    def start(c):
        @pl.when(c < groups)
        def _():
            for q in range(GROUP):
                copy(c, c % BUFFERS, q).start()

    for c in range(BUFFERS - 1):
        start(c)
    acc[...] = jnp.zeros_like(acc)
    row = lax.broadcasted_iota(jnp.int32, (16, 128), 0)
    lane = lax.broadcasted_iota(jnp.int32, (16, 128), 1)
    mask = (lane % 16) == row

    def one_group(c, carry):
        start(c + BUFFERS - 1)
        buf = c % BUFFERS
        for q in range(GROUP):
            copy(c, buf, q).wait()
        nus = []
        for q in range(GROUP):
            at = base + c * GROUP + q
            mu = mu_ref[at]
            nus.append(coeff_ref[pl.ds(pl.multiple_of(nu_ref[at] * 32, 32), 32), :])
            left = jnp.concatenate(
                [jnp.where(mask, jnp.broadcast_to(expand_ref[mu, pl.ds(i, 1), :], (16, 128)), 0.0).astype(jnp.bfloat16) for i in range(occ)], axis=0
            )
            tile = tile_buf[buf, q]
            right = jnp.concatenate([tile[:, :16, :].reshape(128, 128), tile[:, 16:, :].reshape(128, 128)], axis=1)
            part = jnp.dot(left, right, preferred_element_type=jnp.float32).astype(jnp.bfloat16)
            for i in range(occ):
                quarter[q * 32 : q * 32 + 16, i * 128 : (i + 1) * 128] = part[i * 16 : (i + 1) * 16, :128]
                quarter[q * 32 + 16 : q * 32 + 32, i * 128 : (i + 1) * 128] = part[i * 16 : (i + 1) * 16, 128:]
        coeff = jnp.concatenate(nus, axis=0).T[:all_occ]
        acc[...] += jnp.dot(coeff, quarter[...], preferred_element_type=jnp.float32)
        return carry

    lax.fori_loop(0, groups, one_group, 0)
    for i in range(occ):
        out_ref[i] = acc[:, i * kl : (i + 1) * kl].astype(out_ref.dtype)


def prep(mu_blocks, nu_blocks, tile_live, batch_target, batch_count, coeff_rows, stride):
    occ, nbf = coeff_rows.shape
    tiles = mu_blocks.shape[0]
    smem = pl.BlockSpec(memory_space=pltpu.SMEM)
    vmem = pl.BlockSpec(memory_space=pltpu.VMEM)
    lists = jax.ShapeDtypeStruct((SPREAD * stride,), jnp.int32)
    return pl.pallas_call(
        functools.partial(prep_kernel, stride=stride, zero_block=nbf // 32, per_batch=tiles // batch_target.shape[0]),
        out_shape=(lists, lists, lists, jax.ShapeDtypeStruct((SPREAD,), jnp.int32), jax.ShapeDtypeStruct((nbf // 8, 32, 128), jnp.float32)),
        in_specs=[smem] * 5 + [vmem],
        out_specs=(smem, smem, smem, smem, vmem),
        cost_estimate=pl.CostEstimate(flops=2_000_000_000, bytes_accessed=3_300_000, transcendentals=0),
        name="prep",
    )(mu_blocks, nu_blocks, tile_live, batch_target, batch_count, coeff_rows)


def partial_sum(lists, expanded, coeff_all, tiles, occ, all_occ, target, stride, dtype):
    smem = pl.BlockSpec(memory_space=pltpu.SMEM)
    vmem = pl.BlockSpec(memory_space=pltpu.VMEM)
    kl = tiles.shape[3]
    return pl.pallas_call(
        functools.partial(partial_kernel, target=target, stride=stride),
        out_shape=jax.ShapeDtypeStruct((occ, all_occ, kl), dtype),
        in_specs=[smem] * 4 + [pl.BlockSpec(memory_space=pl.ANY), vmem, vmem],
        out_specs=vmem,
        scratch_shapes=[
            pltpu.VMEM((BUFFERS, GROUP, *tiles.shape[1:]), tiles.dtype),
            pltpu.VMEM((GROUP * 32, occ * kl), jnp.bfloat16),
            pltpu.VMEM((all_occ, occ * kl), jnp.float32),
            pltpu.SemaphoreType.DMA((BUFFERS, GROUP)),
        ],
        cost_estimate=pl.CostEstimate(flops=4_000_000_000, bytes_accessed=8_000_000, transcendentals=0),
        name="partial",
    )(*lists, tiles, expanded, coeff_all)


def local(ao_tiles, mo_coeffs, mu_blocks, nu_blocks, tile_live, batch_target, batch_count):
    nbf, occ = mo_coeffs.shape
    ranks = lax.axis_size("occ")
    tasks = lax.axis_size("task")
    all_occ = occ * ranks
    stride = ao_tiles.shape[0] + GROUP
    rows = mo_coeffs.T
    gathered = lax.all_to_all(jnp.broadcast_to(rows[None], (ranks, *rows.shape)), "occ", 0, 0, tiled=True)
    *lists, expanded = prep(mu_blocks, nu_blocks, tile_live, batch_target, batch_count, rows, stride)
    coeff_all = jnp.pad(gathered.reshape(all_occ, nbf).T, ((0, 32), (0, 256 - all_occ)))
    part = functools.partial(partial_sum, lists, expanded, coeff_all, ao_tiles, occ, all_occ, stride=stride)

    ring = 4
    ahead = [(t, (t + 1) % tasks) for t in range(tasks)]
    back = [(t, t // ring * ring + (t - 1) % ring) for t in range(tasks)]
    back_on = [(t // ring * ring + (t - 1) % ring, (t + 2) % tasks) for t in range(tasks)]
    cut = occ // 3

    two = part(target=2, dtype=jnp.bfloat16)
    back_half = lax.ppermute(two[cut:], "task", back)
    chain = lax.ppermute(two[:cut], "task", ahead)
    one = part(target=1, dtype=jnp.bfloat16)
    near = lax.ppermute(one[cut:], "task", ahead)
    zero = part(target=0, dtype=jnp.float32)
    summed = (chain.astype(jnp.float32) + one[:cut].astype(jnp.float32)).astype(jnp.bfloat16)
    last = lax.ppermute(summed, "task", ahead)
    far = lax.ppermute(back_half, "task", back_on)
    return jnp.concatenate([zero[:cut] + last, zero[cut:] + (near.astype(jnp.float32) + far)], axis=0)


def solution(mesh):
    in_specs = (P("task", None, None, None), P(None, "occ"), P("task"), P("task"), P("task"), P("task"), P("task"))
    return jax.shard_map(local, mesh=mesh, in_specs=in_specs, out_specs=P("occ", None, "task"), check_vma=False)
```

```python
import functools

import jax
import jax.numpy as jnp
from jax import lax
from jax.experimental import pallas as pl
from jax.experimental.pallas import tpu as pltpu
from jax.sharding import PartitionSpec as P

SPREAD = 3
GROUP = 8
BUFFERS = 4
NU = 32
VMEM_BYTES = 46 << 20
BF16 = jnp.bfloat16
SMEM = pl.BlockSpec(memory_space=pltpu.SMEM)
VMEM = pl.BlockSpec(memory_space=pltpu.VMEM)
ANY = pl.BlockSpec(memory_space=pl.ANY)


def list_kernel(mu_ref, nu_ref, live_ref, target_ref, count_ref, out_ref, *, stride, zero_block):
    per_batch = mu_ref.shape[0] // target_ref.shape[0]
    size = 3 * stride
    for s in range(SPREAD):
        out_ref[SPREAD * size + s] = 0

    def one_batch(b, carry):
        s = target_ref[b]
        n = out_ref[SPREAD * size + s]
        for q in range(per_batch):
            g = b * per_batch + q
            out_ref[s * size + n] = g
            out_ref[s * size + stride + n] = mu_ref[g]
            out_ref[s * size + 2 * stride + n] = nu_ref[g]
            n = n + live_ref[g]
        out_ref[SPREAD * size + s] = n
        return carry

    lax.fori_loop(0, count_ref[0], one_batch, 0)
    for s in range(SPREAD):
        n = out_ref[SPREAD * size + s]
        for q in range(GROUP):
            out_ref[s * size + n + q] = 0
            out_ref[s * size + stride + n + q] = 0
            out_ref[s * size + 2 * stride + n + q] = zero_block


def expand_rows(rows_ref, padded, expand):
    padded[: rows_ref.shape[0], :] = rows_ref[...]
    chunks = rows_ref.shape[1] // 128
    left = jnp.concatenate([padded[:, c * 128 : (c + 1) * 128] for c in range(chunks)], axis=0)
    row = lax.broadcasted_iota(jnp.int32, (128, 256), 0)
    lane = lax.broadcasted_iota(jnp.int32, (128, 256), 1)
    for pair in range(8):
        select = jnp.where(row == pair * 16 + lane // 16, 1.0, 0.0).astype(BF16)
        wide = jnp.dot(left, select, preferred_element_type=jnp.float32)
        for c in range(chunks):
            for half in range(2):
                expand[c * 16 + pair * 2 + half] = wide[c * 32 : (c + 1) * 32, half * 128 : (half + 1) * 128]


def tile_copies(tiles_ref, lists, base, tile_buf, sems):
    def copy(c, q):
        slot = lists[base + c * GROUP + q]
        return pltpu.make_async_copy(tiles_ref.at[slot], tile_buf.at[c % BUFFERS, q], sems.at[c % BUFFERS, q])

    return copy


def start_tiles(copy, c, groups):
    @pl.when(c < groups)
    def _():
        for q in range(GROUP):
            copy(c, q).start()


def diagonal_mask():
    row = lax.broadcasted_iota(jnp.int32, (16, 128), 0)
    lane = lax.broadcasted_iota(jnp.int32, (16, 128), 1)
    return (lane % 16) == row


def quarter_tile(mask, expand, mu, tile, q, ids, out):
    left = jnp.concatenate(
        [jnp.where(mask, jnp.broadcast_to(expand[mu, pl.ds(i, 1), :], (16, 128)), 0.0).astype(BF16) for i in ids], axis=0
    )
    right = jnp.concatenate([tile[:, :16, :].reshape(128, 128), tile[:, 16:, :].reshape(128, 128)], axis=1)
    part = jnp.dot(left, right, preferred_element_type=jnp.float32).astype(BF16)
    for i in range(len(ids)):
        out[q * NU : q * NU + 16, i * 128 : (i + 1) * 128] = part[i * 16 : (i + 1) * 16, :128]
        out[q * NU + 16 : (q + 1) * NU, i * 128 : (i + 1) * 128] = part[i * 16 : (i + 1) * 16, 128:]


def coeff_group(coeff_ref, lists, at, all_occ):
    blocks = [coeff_ref[pl.ds(pl.multiple_of(lists[at + q] * NU, NU), NU), :] for q in range(GROUP)]
    return jnp.concatenate(blocks, axis=0).T[:all_occ]


def gather_coefficients(blocks, stacked, coeff, occ):
    ranks = len(blocks)
    nbf = stacked.shape[1]
    me = lax.axis_index("occ")
    row = lax.broadcasted_iota(jnp.int32, (32, 256), 0)
    lane = lax.broadcasted_iota(jnp.int32, (32, 256), 1)
    place = []
    for r in range(ranks):
        rank = (me + 2 * (r // 2)) % ranks
        rank = rank + (r % 2) * (1 - 2 * (rank % 2))
        place.append(jnp.where((lane == rank * occ + row) & (row < occ), 1.0, 0.0).astype(BF16))
        stacked[r * 32 : (r + 1) * 32, :] = jnp.zeros((32, nbf), BF16)
        stacked[r * 32 : r * 32 + occ, :] = blocks[r][...]
    place = jnp.concatenate(place, axis=0)
    for c in range(nbf // 256):
        coeff[c * 256 : (c + 1) * 256, :] = jnp.dot(
            stacked[:, c * 256 : (c + 1) * 256].T, place, preferred_element_type=jnp.float32
        ).astype(BF16)
    coeff[nbf:, :] = jnp.zeros((NU, 256), BF16)


def partial_kernel(lists_ref, tiles_ref, rows_ref, *refs, ids, pieces, after, assemble, direct, target, stride, all_occ):
    coeff_refs, refs = refs[: max(assemble, 1)], refs[max(assemble, 1) + after :]
    outs, refs = refs[: len(pieces) + bool(assemble)], refs[len(pieces) + bool(assemble) :]
    lists, rows, padded, expand, tile_buf, quarter, acc, coeff, tile_sems, sems, *rest = refs
    kl = tile_buf.shape[-1]
    lists_in = pltpu.make_async_copy(lists_ref, lists, sems.at[0])
    lists_in.start()
    rows_in = pltpu.make_async_copy(rows_ref, rows, sems.at[1])
    rows_in.start()
    if assemble:
        *blocks, stacked = rest[: assemble + 1]
        rest = rest[assemble + 1 :]
        coeff_in = [pltpu.make_async_copy(ref, block, sems.at[2 + r]) for r, (ref, block) in enumerate(zip(coeff_refs, blocks))]
        coeff_out = pltpu.make_async_copy(coeff, outs[0], sems.at[2])
    else:
        coeff_in = [pltpu.make_async_copy(coeff_refs[0], coeff, sems.at[2])]
    for one in coeff_in:
        one.start()
    acc[...] = jnp.zeros_like(acc)
    base = target * 3 * stride
    lists_in.wait()
    groups = (lists[3 * SPREAD * stride + target] + GROUP - 1) // GROUP
    copy = tile_copies(tiles_ref, lists, base, tile_buf, tile_sems)
    for c in range(BUFFERS - 1):
        start_tiles(copy, c, groups)
    rows_in.wait()
    expand_rows(rows, padded, expand)
    for one in coeff_in:
        one.wait()
    if assemble:
        gather_coefficients(blocks, stacked, coeff, rows.shape[0])
        coeff_out.start()
    mask = diagonal_mask()

    def take(c):
        start_tiles(copy, c + BUFFERS - 1, groups)
        for q in range(GROUP):
            copy(c, q).wait()

    def make_quarter(c):
        for q in range(GROUP):
            quarter_tile(mask, expand, lists[base + stride + c * GROUP + q], tile_buf[c % BUFFERS, q], q, ids, quarter)

    def add_group(c):
        left = coeff_group(coeff, lists, base + 2 * stride + c * GROUP, all_occ)
        acc[...] += jnp.dot(left, quarter[...], preferred_element_type=jnp.float32)

    @pl.when(groups > 0)
    def _():
        take(0)
        make_quarter(0)

    def one_group(c, carry):
        take(c + 1)
        add_group(c)
        make_quarter(c + 1)
        return carry

    lax.fori_loop(0, groups - 1, one_group, 0)

    @pl.when(groups > 0)
    def _():
        add_group(groups - 1)

    puts = []
    at = 0
    for out, piece in zip(outs[bool(assemble) :], pieces):
        for k in range(piece):
            if direct:
                source = acc.at[:, at * kl : (at + 1) * kl]
            else:
                rest[0][at] = acc[:, at * kl : (at + 1) * kl].astype(out.dtype)
                source = rest[0].at[at]
            puts.append(pltpu.make_async_copy(source, out.at[k], rest[-1].at[at]))
            puts[-1].start()
            at += 1
    for put in puts:
        put.wait()
    if assemble:
        coeff_out.wait()


def cost(flops, moved):
    return pl.CostEstimate(flops=flops, bytes_accessed=moved, transcendentals=0)


def lists_of(mu_blocks, nu_blocks, tile_live, batch_target, batch_count, stride, nbf):
    return pl.pallas_call(
        functools.partial(list_kernel, stride=stride, zero_block=nbf // NU),
        out_shape=jax.ShapeDtypeStruct((3 * SPREAD * stride + SPREAD,), jnp.int32),
        in_specs=[SMEM] * 5,
        out_specs=SMEM,
        cost_estimate=cost(2_000_000_000, 10_000),
        name="lists",
    )(mu_blocks, nu_blocks, tile_live, batch_target, batch_count)


def partial_sum(lists, tiles, rows, coeff, all_occ, spans, target, stride, dtype, after=()):
    occ, nbf = rows.shape
    kl = tiles.shape[3]
    ids = [i for low, high in spans for i in range(low, high)]
    pieces = [high - low for low, high in spans]
    assemble = len(coeff) if isinstance(coeff, list) else 0
    direct = dtype == jnp.float32
    shapes = [jax.ShapeDtypeStruct((piece, all_occ, kl), dtype) for piece in pieces]
    scratch = [
        pltpu.SMEM(lists.shape, jnp.int32),
        pltpu.VMEM((occ, nbf), BF16),
        pltpu.VMEM((32, nbf), BF16),
        pltpu.VMEM((nbf // 8, 32, 128), jnp.float32),
        pltpu.VMEM((BUFFERS, GROUP, *tiles.shape[1:]), BF16),
        pltpu.VMEM((GROUP * NU, len(ids) * kl), BF16),
        pltpu.VMEM((all_occ, len(ids) * kl), jnp.float32),
        pltpu.VMEM((nbf + NU, 256), BF16),
        pltpu.SemaphoreType.DMA((BUFFERS, GROUP)),
        pltpu.SemaphoreType.DMA((2 + max(assemble, 1),)),
    ]
    if assemble:
        shapes = [jax.ShapeDtypeStruct((nbf + NU, 256), BF16)] + shapes
        scratch += [pltpu.VMEM(block.shape, BF16) for block in coeff] + [pltpu.VMEM((256, nbf), BF16)]
    if not direct:
        scratch += [pltpu.VMEM((len(ids), all_occ, kl), dtype)]
    scratch += [pltpu.SemaphoreType.DMA((len(ids),))]
    coeff = coeff if assemble else [coeff]
    return pl.pallas_call(
        functools.partial(
            partial_kernel, ids=ids, pieces=pieces, after=len(after), assemble=assemble, direct=direct, target=target, stride=stride, all_occ=all_occ
        ),
        out_shape=tuple(shapes),
        in_specs=[ANY] * (3 + len(coeff) + len(after)),
        out_specs=(ANY,) * len(shapes),
        scratch_shapes=scratch,
        compiler_params=pltpu.CompilerParams(vmem_limit_bytes=VMEM_BYTES if direct else None),
        cost_estimate=cost(6_000_000_000, 10_000_000),
        name="partial",
    )(lists, tiles, rows, *coeff, *after)


def local(ao_tiles, mo_coeffs, mu_blocks, nu_blocks, tile_live, batch_target, batch_count):
    nbf, occ = mo_coeffs.shape
    ranks = lax.axis_size("occ")
    tasks = lax.axis_size("task")
    all_occ = occ * ranks
    stride = ao_tiles.shape[0] + GROUP
    rows = mo_coeffs.T

    others = [lax.ppermute(rows, "occ", [((r + 2 * d) % ranks, r) for r in range(ranks)]) for d in range(1, ranks // 2)]
    lists = lists_of(mu_blocks, nu_blocks, tile_live, batch_target, batch_count, stride, nbf)
    others, lists = lax.optimization_barrier((others, lists))
    blocks = []
    for block in [rows] + others:
        blocks += [block, lax.ppermute(block, "occ", [(r ^ 1, r) for r in range(ranks)])]

    ring = 4
    ahead = [(t, (t + 1) % tasks) for t in range(tasks)]
    back = [(t, t // ring * ring + (t - 1) % ring) for t in range(tasks)]
    back_on = [(t // ring * ring + (t - 1) % ring, (t + 2) % tasks) for t in range(tasks)]
    wide = jnp.float32
    cut, half = 8, 19

    part = functools.partial(partial_sum, lists, ao_tiles, rows, all_occ=all_occ, stride=stride)
    coeff_all, two_low, two_a, two_b = part(coeff=blocks, spans=[(0, cut), (cut, half), (half, occ)], target=2, dtype=BF16)
    back_a = lax.ppermute(two_a, "task", back)
    chain = lax.ppermute(two_low, "task", ahead)
    back_b = lax.ppermute(two_b, "task", back)
    one_low, one_high = part(coeff=coeff_all, spans=[(0, cut), (cut, occ)], target=1, dtype=BF16)
    near = lax.ppermute(one_high, "task", ahead)
    far_a = lax.ppermute(back_a, "task", back_on)
    summed = (chain.astype(wide) + one_low.astype(wide)).astype(BF16)
    last = lax.ppermute(summed, "task", ahead)
    (out,) = part(coeff=coeff_all, spans=[(0, occ)], target=0, dtype=wide, after=(back_b,))
    far_b = lax.ppermute(back_b, "task", back_on)
    added = jnp.concatenate([last.astype(wide), near[: half - cut].astype(wide) + far_a.astype(wide), near[half - cut :].astype(wide) + far_b.astype(wide)])
    return out + added


def solution(mesh):
    in_specs = (P("task", None, None, None), P(None, "occ"), P("task"), P("task"), P("task"), P("task"), P("task"))
    return jax.shard_map(local, mesh=mesh, in_specs=in_specs, out_specs=P("occ", None, "task"), check_vma=False)
```

```python
import functools

import jax
import jax.numpy as jnp
from jax import lax
from jax.experimental import pallas as pl
from jax.experimental.pallas import tpu as pltpu
from jax.sharding import PartitionSpec as P

SPREAD = 3
GROUP = 8
BUFFERS = 4
NU = 32
VMEM_BYTES = 46 << 20
BF16 = jnp.bfloat16
SMEM = pl.BlockSpec(memory_space=pltpu.SMEM)
VMEM = pl.BlockSpec(memory_space=pltpu.VMEM)
ANY = pl.BlockSpec(memory_space=pl.ANY)


def list_kernel(mu_ref, nu_ref, live_ref, target_ref, count_ref, out_ref, *, stride, zero_block):
    per_batch = mu_ref.shape[0] // target_ref.shape[0]
    size = 3 * stride
    for s in range(SPREAD):
        out_ref[SPREAD * size + s] = 0

    def one_batch(b, carry):
        s = target_ref[b]
        n = out_ref[SPREAD * size + s]
        for q in range(per_batch):
            g = b * per_batch + q
            out_ref[s * size + n] = g
            out_ref[s * size + stride + n] = mu_ref[g]
            out_ref[s * size + 2 * stride + n] = nu_ref[g]
            n = n + live_ref[g]
        out_ref[SPREAD * size + s] = n
        return carry

    lax.fori_loop(0, count_ref[0], one_batch, 0)
    for s in range(SPREAD):
        n = out_ref[SPREAD * size + s]
        for q in range(GROUP):
            out_ref[s * size + n + q] = 0
            out_ref[s * size + stride + n + q] = 0
            out_ref[s * size + 2 * stride + n + q] = zero_block


def expand_rows(rows_ref, padded, expand):
    padded[: rows_ref.shape[0], :] = rows_ref[...]
    chunks = rows_ref.shape[1] // 128
    left = jnp.concatenate([padded[:, c * 128 : (c + 1) * 128] for c in range(chunks)], axis=0)
    row = lax.broadcasted_iota(jnp.int32, (128, 256), 0)
    lane = lax.broadcasted_iota(jnp.int32, (128, 256), 1)
    for pair in range(8):
        select = jnp.where(row == pair * 16 + lane // 16, 1.0, 0.0).astype(BF16)
        wide = jnp.dot(left, select, preferred_element_type=jnp.float32)
        for c in range(chunks):
            for half in range(2):
                expand[c * 16 + pair * 2 + half] = wide[c * 32 : (c + 1) * 32, half * 128 : (half + 1) * 128]


def tile_copies(tiles_ref, lists, base, tile_buf, sems):
    def copy(c, q):
        slot = lists[base + c * GROUP + q]
        return pltpu.make_async_copy(tiles_ref.at[slot], tile_buf.at[c % BUFFERS, q], sems.at[c % BUFFERS, q])

    return copy


def start_tiles(copy, c, groups):
    @pl.when(c < groups)
    def _():
        for q in range(GROUP):
            copy(c, q).start()


def diagonal_mask():
    row = lax.broadcasted_iota(jnp.int32, (16, 128), 0)
    lane = lax.broadcasted_iota(jnp.int32, (16, 128), 1)
    return (lane % 16) == row


def quarter_tile(mask, expand, mu, tile, q, ids, out):
    left = jnp.concatenate(
        [jnp.where(mask, jnp.broadcast_to(expand[mu, pl.ds(i, 1), :], (16, 128)), 0.0).astype(BF16) for i in ids], axis=0
    )
    right = jnp.concatenate([tile[:, :16, :].reshape(128, 128), tile[:, 16:, :].reshape(128, 128)], axis=1)
    part = jnp.dot(left, right, preferred_element_type=jnp.float32).astype(BF16)
    for i in range(len(ids)):
        out[q * NU : q * NU + 16, i * 128 : (i + 1) * 128] = part[i * 16 : (i + 1) * 16, :128]
        out[q * NU + 16 : (q + 1) * NU, i * 128 : (i + 1) * 128] = part[i * 16 : (i + 1) * 16, 128:]


def coeff_group(coeff_ref, lists, at, all_occ):
    blocks = [coeff_ref[pl.ds(pl.multiple_of(lists[at + q] * NU, NU), NU), :] for q in range(GROUP)]
    return jnp.concatenate(blocks, axis=0).T[:all_occ]


def gather_coefficients(blocks, stacked, coeff, occ):
    ranks = len(blocks)
    nbf = stacked.shape[1]
    me = lax.axis_index("occ")
    row = lax.broadcasted_iota(jnp.int32, (32, 256), 0)
    lane = lax.broadcasted_iota(jnp.int32, (32, 256), 1)
    place = []
    for r in range(ranks):
        rank = (me + 2 * (r // 2)) % ranks
        rank = rank + (r % 2) * (1 - 2 * (rank % 2))
        place.append(jnp.where((lane == rank * occ + row) & (row < occ), 1.0, 0.0).astype(BF16))
        stacked[r * 32 : (r + 1) * 32, :] = jnp.zeros((32, nbf), BF16)
        stacked[r * 32 : r * 32 + occ, :] = blocks[r][...]
    place = jnp.concatenate(place, axis=0)
    for c in range(nbf // 256):
        coeff[c * 256 : (c + 1) * 256, :] = jnp.dot(
            stacked[:, c * 256 : (c + 1) * 256].T, place, preferred_element_type=jnp.float32
        ).astype(BF16)
    coeff[nbf:, :] = jnp.zeros((NU, 256), BF16)


def partial_kernel(lists_ref, tiles_ref, rows_ref, *refs, ids, pieces, after, assemble, direct, target, stride, all_occ):
    coeff_refs, refs = refs[: max(assemble, 1)], refs[max(assemble, 1) + after :]
    outs, refs = refs[: len(pieces) + bool(assemble)], refs[len(pieces) + bool(assemble) :]
    coeff_all, outs = (outs[0], outs[1:]) if assemble else (None, outs)
    lists, rows, padded, expand, tile_buf, quarter, acc, coeff, tile_sems, sems, *rest = refs
    kl = tile_buf.shape[-1]
    lists_in = pltpu.make_async_copy(lists_ref, lists, sems.at[0])
    lists_in.start()
    rows_in = pltpu.make_async_copy(rows_ref, rows, sems.at[1])
    rows_in.start()
    if assemble:
        *blocks, stacked = rest[: assemble + 1]
        rest = rest[assemble + 1 :]
        coeff_in = [pltpu.make_async_copy(ref, block, sems.at[2 + r]) for r, (ref, block) in enumerate(zip(coeff_refs, blocks))]
        coeff_out = pltpu.make_async_copy(coeff, coeff_all, sems.at[2])
    else:
        coeff_in = [pltpu.make_async_copy(coeff_refs[0], coeff, sems.at[2])]
    for one in coeff_in:
        one.start()
    acc[...] = jnp.zeros_like(acc)
    base = target * 3 * stride
    lists_in.wait()
    groups = (lists[3 * SPREAD * stride + target] + GROUP - 1) // GROUP
    copy = tile_copies(tiles_ref, lists, base, tile_buf, tile_sems)
    for c in range(BUFFERS - 1):
        start_tiles(copy, c, groups)
    rows_in.wait()
    expand_rows(rows, padded, expand)
    for one in coeff_in:
        one.wait()
    if assemble:
        gather_coefficients(blocks, stacked, coeff, rows.shape[0])
        coeff_out.start()
    mask = diagonal_mask()

    def take(c):
        start_tiles(copy, c + BUFFERS - 1, groups)
        for q in range(GROUP):
            copy(c, q).wait()

    def make_quarter(c):
        for q in range(GROUP):
            quarter_tile(mask, expand, lists[base + stride + c * GROUP + q], tile_buf[c % BUFFERS, q], q, ids, quarter)

    def add_group(c):
        left = coeff_group(coeff, lists, base + 2 * stride + c * GROUP, all_occ)
        acc[...] += jnp.dot(left, quarter[...], preferred_element_type=jnp.float32)

    @pl.when(groups > 0)
    def _():
        take(0)
        make_quarter(0)

    def one_group(c, carry):
        take(c + 1)
        add_group(c)
        make_quarter(c + 1)
        return carry

    lax.fori_loop(0, groups - 1, one_group, 0)

    puts = []
    at = 0
    for out, piece in zip(outs, pieces):
        for k in range(piece):
            source = acc.at[:, (at + k) * kl : (at + k + 1) * kl] if direct else rest[0].at[at + k]
            puts.append(pltpu.make_async_copy(source, out.at[k], rest[-1].at[at + k]))
        at += piece

    def finish(total):
        at = 0
        for piece in pieces:
            value = total(slice(at * kl, (at + piece) * kl))
            for k in range(piece):
                if direct:
                    acc[:, (at + k) * kl : (at + k + 1) * kl] = value[:, k * kl : (k + 1) * kl]
                else:
                    rest[0][at + k] = value[:, k * kl : (k + 1) * kl].astype(rest[0].dtype)
                puts[at + k].start()
            at += piece

    @pl.when(groups > 0)
    def _():
        left = coeff_group(coeff, lists, base + 2 * stride + (groups - 1) * GROUP, all_occ)
        finish(lambda cols: acc[:, cols] + jnp.dot(left, quarter[:, cols], preferred_element_type=jnp.float32))

    @pl.when(groups == 0)
    def _():
        finish(lambda cols: acc[:, cols])

    for put in puts:
        put.wait()
    if assemble:
        coeff_out.wait()


def cost(flops, moved):
    return pl.CostEstimate(flops=flops, bytes_accessed=moved, transcendentals=0)


def lists_of(mu_blocks, nu_blocks, tile_live, batch_target, batch_count, stride, nbf):
    return pl.pallas_call(
        functools.partial(list_kernel, stride=stride, zero_block=nbf // NU),
        out_shape=jax.ShapeDtypeStruct((3 * SPREAD * stride + SPREAD,), jnp.int32),
        in_specs=[SMEM] * 5,
        out_specs=SMEM,
        cost_estimate=cost(2_000_000_000, 10_000),
        name="lists",
    )(mu_blocks, nu_blocks, tile_live, batch_target, batch_count)


def partial_sum(lists, tiles, rows, coeff, all_occ, spans, target, stride, dtype, after=()):
    occ, nbf = rows.shape
    kl = tiles.shape[3]
    ids = [i for low, high in spans for i in range(low, high)]
    pieces = [high - low for low, high in spans]
    assemble = len(coeff) if isinstance(coeff, list) else 0
    direct = dtype == jnp.float32
    shapes = [jax.ShapeDtypeStruct((piece, all_occ, kl), dtype) for piece in pieces]
    scratch = [
        pltpu.SMEM(lists.shape, jnp.int32),
        pltpu.VMEM((occ, nbf), BF16),
        pltpu.VMEM((32, nbf), BF16),
        pltpu.VMEM((nbf // 8, 32, 128), jnp.float32),
        pltpu.VMEM((BUFFERS, GROUP, *tiles.shape[1:]), BF16),
        pltpu.VMEM((GROUP * NU, len(ids) * kl), BF16),
        pltpu.VMEM((all_occ, len(ids) * kl), jnp.float32),
        pltpu.VMEM((nbf + NU, 256), BF16),
        pltpu.SemaphoreType.DMA((BUFFERS, GROUP)),
        pltpu.SemaphoreType.DMA((2 + max(assemble, 1),)),
    ]
    if assemble:
        shapes = [jax.ShapeDtypeStruct((nbf + NU, 256), BF16)] + shapes
        scratch += [pltpu.VMEM(block.shape, BF16) for block in coeff] + [pltpu.VMEM((256, nbf), BF16)]
    if not direct:
        scratch += [pltpu.VMEM((len(ids), all_occ, kl), dtype)]
    scratch += [pltpu.SemaphoreType.DMA((len(ids),))]
    coeff = coeff if assemble else [coeff]
    return pl.pallas_call(
        functools.partial(
            partial_kernel, ids=ids, pieces=pieces, after=len(after), assemble=assemble, direct=direct, target=target, stride=stride, all_occ=all_occ
        ),
        out_shape=tuple(shapes),
        in_specs=[ANY] * (3 + len(coeff) + len(after)),
        out_specs=(ANY,) * len(shapes),
        scratch_shapes=scratch,
        compiler_params=pltpu.CompilerParams(vmem_limit_bytes=VMEM_BYTES if direct else None),
        cost_estimate=cost(6_000_000_000, 10_000_000),
        name="partial",
    )(lists, tiles, rows, *coeff, *after)


def local(ao_tiles, mo_coeffs, mu_blocks, nu_blocks, tile_live, batch_target, batch_count):
    nbf, occ = mo_coeffs.shape
    ranks = lax.axis_size("occ")
    tasks = lax.axis_size("task")
    all_occ = occ * ranks
    stride = ao_tiles.shape[0] + GROUP
    rows = mo_coeffs.T

    others = [lax.ppermute(rows, "occ", [((r + 2 * d) % ranks, r) for r in range(ranks)]) for d in range(1, ranks // 2)]
    lists = lists_of(mu_blocks, nu_blocks, tile_live, batch_target, batch_count, stride, nbf)
    others, lists = lax.optimization_barrier((others, lists))
    blocks = []
    for block in [rows] + others:
        blocks += [block, lax.ppermute(block, "occ", [(r ^ 1, r) for r in range(ranks)])]

    ring = 4
    ahead = [(t, (t + 1) % tasks) for t in range(tasks)]
    back = [(t, t // ring * ring + (t - 1) % ring) for t in range(tasks)]
    back_on = [(t // ring * ring + (t - 1) % ring, (t + 2) % tasks) for t in range(tasks)]
    wide = jnp.float32
    cut, half = 8, 19

    part = functools.partial(partial_sum, lists, ao_tiles, rows, all_occ=all_occ, stride=stride)
    coeff_all, two_low, two_a, two_b = part(coeff=blocks, spans=[(0, cut), (cut, half), (half, occ)], target=2, dtype=BF16)
    back_a = lax.ppermute(two_a, "task", back)
    chain = lax.ppermute(two_low, "task", ahead)
    back_b = lax.ppermute(two_b, "task", back)
    one_low, one_high = part(coeff=coeff_all, spans=[(0, cut), (cut, occ)], target=1, dtype=BF16)
    near = lax.ppermute(one_high, "task", ahead)
    far_a = lax.ppermute(back_a, "task", back_on)
    summed = (chain.astype(wide) + one_low.astype(wide)).astype(BF16)
    last = lax.ppermute(summed, "task", ahead)
    (out,) = part(coeff=coeff_all, spans=[(0, occ)], target=0, dtype=wide, after=(back_b,))
    far_b = lax.ppermute(back_b, "task", back_on)
    added = jnp.concatenate([last.astype(wide), near[: half - cut].astype(wide) + far_a.astype(wide), near[half - cut :].astype(wide) + far_b.astype(wide)])
    return out + added


def solution(mesh):
    in_specs = (P("task", None, None, None), P(None, "occ"), P("task"), P("task"), P("task"), P("task"), P("task"))
    return jax.shard_map(local, mesh=mesh, in_specs=in_specs, out_specs=P("occ", None, "task"), check_vma=False)
```

```python
import functools

import jax
import jax.numpy as jnp
from jax import lax
from jax.experimental import pallas as pl
from jax.experimental.pallas import tpu as pltpu
from jax.sharding import PartitionSpec as P


SPREAD = 3
GROUP = 8
BUFFERS = 4
NU = 32
VMEM_BYTES = 46 << 20
BF16 = jnp.bfloat16
SMEM = pl.BlockSpec(memory_space=pltpu.SMEM)
VMEM = pl.BlockSpec(memory_space=pltpu.VMEM)
ANY = pl.BlockSpec(memory_space=pl.ANY)


def list_kernel(mu_ref, nu_ref, live_ref, target_ref, count_ref, out_ref, *, stride, zero_block):
    per_batch = mu_ref.shape[0] // target_ref.shape[0]
    size = 3 * stride
    for s in range(SPREAD):
        out_ref[SPREAD * size + s] = 0

    def one_batch(b, carry):
        s = target_ref[b]
        n = out_ref[SPREAD * size + s]
        for q in range(per_batch):
            g = b * per_batch + q
            out_ref[s * size + n] = g
            out_ref[s * size + stride + n] = mu_ref[g]
            out_ref[s * size + 2 * stride + n] = nu_ref[g]
            n = n + live_ref[g]
        out_ref[SPREAD * size + s] = n
        return carry

    lax.fori_loop(0, count_ref[0], one_batch, 0)
    for s in range(SPREAD):
        n = out_ref[SPREAD * size + s]
        for q in range(GROUP):
            out_ref[s * size + n + q] = 0
            out_ref[s * size + stride + n + q] = 0
            out_ref[s * size + 2 * stride + n + q] = zero_block


def expand_rows(rows_ref, padded, expand):
    padded[: rows_ref.shape[0], :] = rows_ref[...]
    chunks = rows_ref.shape[1] // 128
    left = jnp.concatenate([padded[:, c * 128 : (c + 1) * 128] for c in range(chunks)], axis=0)
    row = lax.broadcasted_iota(jnp.int32, (128, 256), 0)
    lane = lax.broadcasted_iota(jnp.int32, (128, 256), 1)
    for pair in range(8):
        select = jnp.where(row == pair * 16 + lane // 16, 1.0, 0.0).astype(BF16)
        wide = jnp.dot(left, select, preferred_element_type=jnp.float32)
        for c in range(chunks):
            for half in range(2):
                expand[c * 16 + pair * 2 + half] = wide[c * 32 : (c + 1) * 32, half * 128 : (half + 1) * 128]


def tile_copies(tiles_ref, lists, base, tile_buf, sems):
    def copy(c, q):
        slot = lists[base + c * GROUP + q]
        return pltpu.make_async_copy(tiles_ref.at[slot], tile_buf.at[c % BUFFERS, q], sems.at[c % BUFFERS, q])

    return copy


def start_tiles(copy, c, groups):
    @pl.when(c < groups)
    def _():
        for q in range(GROUP):
            copy(c, q).start()


def diagonal_mask():
    row = lax.broadcasted_iota(jnp.int32, (16, 128), 0)
    lane = lax.broadcasted_iota(jnp.int32, (16, 128), 1)
    return (lane % 16) == row


def quarter_tile(mask, expand, mu, tile, q, ids, out):
    left = jnp.concatenate(
        [jnp.where(mask, jnp.broadcast_to(expand[mu, pl.ds(i, 1), :], (16, 128)), 0.0).astype(BF16) for i in ids], axis=0
    )
    right = jnp.concatenate([tile[:, :16, :].reshape(128, 128), tile[:, 16:, :].reshape(128, 128)], axis=1)
    part = jnp.dot(left, right, preferred_element_type=jnp.float32).astype(BF16)
    for i in range(len(ids)):
        out[q * NU : q * NU + 16, i * 128 : (i + 1) * 128] = part[i * 16 : (i + 1) * 16, :128]
        out[q * NU + 16 : (q + 1) * NU, i * 128 : (i + 1) * 128] = part[i * 16 : (i + 1) * 16, 128:]


def coeff_group(coeff_ref, lists, at, all_occ):
    blocks = [coeff_ref[pl.ds(pl.multiple_of(lists[at + q] * NU, NU), NU), :] for q in range(GROUP)]
    return jnp.concatenate(blocks, axis=0).T[:all_occ]


def gather_coefficients(blocks, stacked, coeff, occ):
    ranks = len(blocks)
    nbf = stacked.shape[1]
    me = lax.axis_index("occ")
    row = lax.broadcasted_iota(jnp.int32, (32, 256), 0)
    lane = lax.broadcasted_iota(jnp.int32, (32, 256), 1)
    place = []
    for r in range(ranks):
        rank = (me + 2 * (r // 2)) % ranks
        rank = rank + (r % 2) * (1 - 2 * (rank % 2))
        place.append(jnp.where((lane == rank * occ + row) & (row < occ), 1.0, 0.0).astype(BF16))
        stacked[r * 32 : (r + 1) * 32, :] = jnp.zeros((32, nbf), BF16)
        stacked[r * 32 : r * 32 + occ, :] = blocks[r][...]
    place = jnp.concatenate(place, axis=0)
    for c in range(nbf // 256):
        coeff[c * 256 : (c + 1) * 256, :] = jnp.dot(
            stacked[:, c * 256 : (c + 1) * 256].T, place, preferred_element_type=jnp.float32
        ).astype(BF16)
    coeff[nbf:, :] = jnp.zeros((NU, 256), BF16)


def partial_kernel(lists_ref, tiles_ref, rows_ref, *refs, ids, pieces, after, assemble, direct, target, stride, all_occ):
    coeff_refs, refs = refs[: max(assemble, 1)], refs[max(assemble, 1) + after :]
    outs, refs = refs[: len(pieces) + bool(assemble)], refs[len(pieces) + bool(assemble) :]
    coeff_all, outs = (outs[0], outs[1:]) if assemble else (None, outs)
    lists, rows, padded, expand, tile_buf, quarter, acc, coeff, tile_sems, sems, *rest = refs
    kl = tile_buf.shape[-1]
    lists_in = pltpu.make_async_copy(lists_ref, lists, sems.at[0])
    lists_in.start()
    rows_in = pltpu.make_async_copy(rows_ref, rows, sems.at[1])
    rows_in.start()
    if assemble:
        *blocks, stacked = rest[: assemble + 1]
        rest = rest[assemble + 1 :]
        coeff_in = [pltpu.make_async_copy(ref, block, sems.at[2 + r]) for r, (ref, block) in enumerate(zip(coeff_refs, blocks))]
        coeff_out = pltpu.make_async_copy(coeff, coeff_all, sems.at[2])
    else:
        coeff_in = [pltpu.make_async_copy(coeff_refs[0], coeff, sems.at[2])]
    for one in coeff_in:
        one.start()
    acc[...] = jnp.zeros_like(acc)
    base = target * 3 * stride
    lists_in.wait()
    groups = (lists[3 * SPREAD * stride + target] + GROUP - 1) // GROUP
    copy = tile_copies(tiles_ref, lists, base, tile_buf, tile_sems)
    for c in range(BUFFERS - 1):
        start_tiles(copy, c, groups)
    rows_in.wait()
    expand_rows(rows, padded, expand)
    for one in coeff_in:
        one.wait()
    if assemble:
        gather_coefficients(blocks, stacked, coeff, rows.shape[0])
        coeff_out.start()
    mask = diagonal_mask()

    def take(c):
        start_tiles(copy, c + BUFFERS - 1, groups)
        for q in range(GROUP):
            copy(c, q).wait()

    def make_quarter(c):
        for q in range(GROUP):
            quarter_tile(mask, expand, lists[base + stride + c * GROUP + q], tile_buf[c % BUFFERS, q], q, ids, quarter)

    def add_group(c):
        left = coeff_group(coeff, lists, base + 2 * stride + c * GROUP, all_occ)
        acc[...] += jnp.dot(left, quarter[...], preferred_element_type=jnp.float32)

    @pl.when(groups > 0)
    def _():
        take(0)
        make_quarter(0)

    def one_group(c, carry):
        take(c + 1)
        add_group(c)
        make_quarter(c + 1)
        return carry

    lax.fori_loop(0, groups - 1, one_group, 0)

    puts = []
    at = 0
    for out, piece in zip(outs, pieces):
        for k in range(piece):
            source = acc.at[:, (at + k) * kl : (at + k + 1) * kl] if direct else rest[0].at[at + k]
            puts.append(pltpu.make_async_copy(source, out.at[k], rest[-1].at[at + k]))
        at += piece

    def finish(total):
        at = 0
        for piece in pieces:
            value = total(slice(at * kl, (at + piece) * kl))
            for k in range(piece):
                if direct:
                    acc[:, (at + k) * kl : (at + k + 1) * kl] = value[:, k * kl : (k + 1) * kl]
                else:
                    rest[0][at + k] = value[:, k * kl : (k + 1) * kl].astype(rest[0].dtype)
                puts[at + k].start()
            at += piece

    @pl.when(groups > 0)
    def _():
        left = coeff_group(coeff, lists, base + 2 * stride + (groups - 1) * GROUP, all_occ)
        finish(lambda cols: acc[:, cols] + jnp.dot(left, quarter[:, cols], preferred_element_type=jnp.float32))

    @pl.when(groups == 0)
    def _():
        finish(lambda cols: acc[:, cols])

    for put in puts:
        put.wait()
    if assemble:
        coeff_out.wait()


def cost(flops, moved):
    return pl.CostEstimate(flops=flops, bytes_accessed=moved, transcendentals=0)


def lists_of(mu_blocks, nu_blocks, tile_live, batch_target, batch_count, stride, nbf):
    return pl.pallas_call(
        functools.partial(list_kernel, stride=stride, zero_block=nbf // NU),
        out_shape=jax.ShapeDtypeStruct((3 * SPREAD * stride + SPREAD,), jnp.int32),
        in_specs=[SMEM] * 5,
        out_specs=SMEM,
        cost_estimate=cost(2_000_000_000, 10_000),
        name="lists",
    )(mu_blocks, nu_blocks, tile_live, batch_target, batch_count)


def partial_sum(lists, tiles, rows, coeff, all_occ, spans, target, stride, dtype, after=()):
    occ, nbf = rows.shape
    kl = tiles.shape[3]
    ids = [i for low, high in spans for i in range(low, high)]
    pieces = [high - low for low, high in spans]
    assemble = len(coeff) if isinstance(coeff, list) else 0
    direct = dtype == jnp.float32
    shapes = [jax.ShapeDtypeStruct((piece, all_occ, kl), dtype) for piece in pieces]
    scratch = [
        pltpu.SMEM(lists.shape, jnp.int32),
        pltpu.VMEM((occ, nbf), BF16),
        pltpu.VMEM((32, nbf), BF16),
        pltpu.VMEM((nbf // 8, 32, 128), jnp.float32),
        pltpu.VMEM((BUFFERS, GROUP, *tiles.shape[1:]), BF16),
        pltpu.VMEM((GROUP * NU, len(ids) * kl), BF16),
        pltpu.VMEM((all_occ, len(ids) * kl), jnp.float32),
        pltpu.VMEM((nbf + NU, 256), BF16),
        pltpu.SemaphoreType.DMA((BUFFERS, GROUP)),
        pltpu.SemaphoreType.DMA((2 + max(assemble, 1),)),
    ]
    if assemble:
        shapes = [jax.ShapeDtypeStruct((nbf + NU, 256), BF16)] + shapes
        scratch += [pltpu.VMEM(block.shape, BF16) for block in coeff] + [pltpu.VMEM((256, nbf), BF16)]
    if not direct:
        scratch += [pltpu.VMEM((len(ids), all_occ, kl), dtype)]
    scratch += [pltpu.SemaphoreType.DMA((len(ids),))]
    coeff = coeff if assemble else [coeff]
    return pl.pallas_call(
        functools.partial(
            partial_kernel, ids=ids, pieces=pieces, after=len(after), assemble=assemble, direct=direct, target=target, stride=stride, all_occ=all_occ
        ),
        out_shape=tuple(shapes),
        in_specs=[ANY] * (3 + len(coeff) + len(after)),
        out_specs=(ANY,) * len(shapes),
        scratch_shapes=scratch,
        compiler_params=pltpu.CompilerParams(vmem_limit_bytes=VMEM_BYTES if direct else None),
        cost_estimate=cost(6_000_000_000, 10_000_000),
        name="partial",
    )(lists, tiles, rows, *coeff, *after)


def local(ao_tiles, mo_coeffs, mu_blocks, nu_blocks, tile_live, batch_target, batch_count):
    nbf, occ = mo_coeffs.shape
    ranks = lax.axis_size("occ")
    tasks = lax.axis_size("task")
    all_occ = occ * ranks
    stride = ao_tiles.shape[0] + GROUP
    rows = mo_coeffs.T

    others = [lax.ppermute(rows, "occ", [((r + 2 * d) % ranks, r) for r in range(ranks)]) for d in range(1, ranks // 2)]
    lists = lists_of(mu_blocks, nu_blocks, tile_live, batch_target, batch_count, stride, nbf)
    others, lists = lax.optimization_barrier((others, lists))
    blocks = []
    for block in [rows] + others:
        blocks += [block, lax.ppermute(block, "occ", [(r ^ 1, r) for r in range(ranks)])]

    ring = 4
    ahead = [(t, (t + 1) % tasks) for t in range(tasks)]
    back = [(t, t // ring * ring + (t - 1) % ring) for t in range(tasks)]
    back_on = [(t // ring * ring + (t - 1) % ring, (t + 2) % tasks) for t in range(tasks)]
    wide = jnp.float32
    cut, half = 8, 19

    def part(**kwargs):
        return partial_sum(lists, ao_tiles, rows, all_occ=all_occ, stride=stride, **kwargs)

    def sent(array, route):
        return lax.ppermute(array, "task", route)

    coeff_all, two_low, two_a, two_b = part(coeff=blocks, spans=[(0, cut), (cut, half), (half, occ)], target=2, dtype=BF16)
    back_a = sent(two_a, back)
    chain = sent(two_low, ahead)
    back_b = sent(two_b, back)
    (one_high,) = part(coeff=coeff_all, spans=[(cut, occ)], target=1, dtype=BF16)
    (one_low,) = part(coeff=coeff_all, spans=[(0, cut)], target=1, dtype=BF16, after=(one_high,))
    near = sent(one_high, ahead)
    far_a = sent(back_a, back_on)
    summed = (chain.astype(wide) + one_low.astype(wide)).astype(BF16)
    last = sent(summed, ahead)
    far_b = sent(back_b, back_on)
    (out,) = part(coeff=coeff_all, spans=[(0, occ)], target=0, dtype=wide, after=(back_a,))
    added = jnp.concatenate([last.astype(wide), near[: half - cut].astype(wide) + far_a.astype(wide), near[half - cut :].astype(wide) + far_b.astype(wide)])
    return out + added


def solution(mesh):
    in_specs = (P("task", None, None, None), P(None, "occ"), P("task"), P("task"), P("task"), P("task"), P("task"))
    return jax.shard_map(local, mesh=mesh, in_specs=in_specs, out_specs=P("occ", None, "task"), check_vma=False)
```

```python
import functools

import jax
import jax.numpy as jnp
from jax import lax
from jax.experimental import pallas as pl
from jax.experimental.pallas import tpu as pltpu
from jax.sharding import PartitionSpec as P


SPREAD = 3
GROUP = 8
BUFFERS = 4
NU = 32
VMEM_BYTES = 46 << 20
BF16 = jnp.bfloat16
SMEM = pl.BlockSpec(memory_space=pltpu.SMEM)
VMEM = pl.BlockSpec(memory_space=pltpu.VMEM)
ANY = pl.BlockSpec(memory_space=pl.ANY)


def list_kernel(mu_ref, nu_ref, live_ref, target_ref, count_ref, out_ref, *, stride, zero_block):
    per_batch = mu_ref.shape[0] // target_ref.shape[0]
    size = 3 * stride
    for s in range(SPREAD):
        out_ref[SPREAD * size + s] = 0

    def one_batch(b, carry):
        s = target_ref[b]
        n = out_ref[SPREAD * size + s]
        for q in range(per_batch):
            g = b * per_batch + q
            out_ref[s * size + n] = g
            out_ref[s * size + stride + n] = mu_ref[g]
            out_ref[s * size + 2 * stride + n] = nu_ref[g]
            n = n + live_ref[g]
        out_ref[SPREAD * size + s] = n
        return carry

    lax.fori_loop(0, count_ref[0], one_batch, 0)
    for s in range(SPREAD):
        n = out_ref[SPREAD * size + s]
        for q in range(GROUP):
            out_ref[s * size + n + q] = 0
            out_ref[s * size + stride + n + q] = 0
            out_ref[s * size + 2 * stride + n + q] = zero_block


def expand_rows(rows_ref, padded, expand):
    padded[: rows_ref.shape[0], :] = rows_ref[...]
    chunks = rows_ref.shape[1] // 128
    left = jnp.concatenate([padded[:, c * 128 : (c + 1) * 128] for c in range(chunks)], axis=0)
    row = lax.broadcasted_iota(jnp.int32, (128, 256), 0)
    lane = lax.broadcasted_iota(jnp.int32, (128, 256), 1)
    for pair in range(8):
        select = jnp.where(row == pair * 16 + lane // 16, 1.0, 0.0).astype(BF16)
        wide = jnp.dot(left, select, preferred_element_type=jnp.float32)
        for c in range(chunks):
            for half in range(2):
                expand[c * 16 + pair * 2 + half] = wide[c * 32 : (c + 1) * 32, half * 128 : (half + 1) * 128]


def tile_copies(tiles_ref, lists, base, tile_buf, sems):
    def copy(c, q):
        slot = lists[base + c * GROUP + q]
        return pltpu.make_async_copy(tiles_ref.at[slot], tile_buf.at[c % BUFFERS, q], sems.at[c % BUFFERS, q])

    return copy


def start_tiles(copy, c, groups):
    @pl.when(c < groups)
    def _():
        for q in range(GROUP):
            copy(c, q).start()


def diagonal_mask():
    row = lax.broadcasted_iota(jnp.int32, (16, 128), 0)
    lane = lax.broadcasted_iota(jnp.int32, (16, 128), 1)
    return (lane % 16) == row


def quarter_tile(mask, expand, mu, tile, q, ids, out):
    left = jnp.concatenate(
        [jnp.where(mask, jnp.broadcast_to(expand[mu, pl.ds(i, 1), :], (16, 128)), 0.0).astype(BF16) for i in ids], axis=0
    )
    right = jnp.concatenate([tile[:, :16, :].reshape(128, 128), tile[:, 16:, :].reshape(128, 128)], axis=1)
    part = jnp.dot(left, right, preferred_element_type=jnp.float32).astype(BF16)
    for i in range(len(ids)):
        out[q * NU : q * NU + 16, i * 128 : (i + 1) * 128] = part[i * 16 : (i + 1) * 16, :128]
        out[q * NU + 16 : (q + 1) * NU, i * 128 : (i + 1) * 128] = part[i * 16 : (i + 1) * 16, 128:]


def coeff_group(coeff_ref, lists, at, all_occ):
    blocks = [coeff_ref[pl.ds(pl.multiple_of(lists[at + q] * NU, NU), NU), :] for q in range(GROUP)]
    return jnp.concatenate(blocks, axis=0).T[:all_occ]


def gather_coefficients(blocks, stacked, coeff, occ):
    ranks = len(blocks)
    nbf = stacked.shape[1]
    me = lax.axis_index("occ")
    row = lax.broadcasted_iota(jnp.int32, (32, 256), 0)
    lane = lax.broadcasted_iota(jnp.int32, (32, 256), 1)
    place = []
    for r in range(ranks):
        rank = (me + 2 * (r // 2)) % ranks
        rank = rank + (r % 2) * (1 - 2 * (rank % 2))
        place.append(jnp.where((lane == rank * occ + row) & (row < occ), 1.0, 0.0).astype(BF16))
        stacked[r * 32 : (r + 1) * 32, :] = jnp.zeros((32, nbf), BF16)
        stacked[r * 32 : r * 32 + occ, :] = blocks[r][...]
    place = jnp.concatenate(place, axis=0)
    for c in range(nbf // 256):
        coeff[c * 256 : (c + 1) * 256, :] = jnp.dot(
            stacked[:, c * 256 : (c + 1) * 256].T, place, preferred_element_type=jnp.float32
        ).astype(BF16)
    coeff[nbf:, :] = jnp.zeros((NU, 256), BF16)


def partial_kernel(lists_ref, tiles_ref, rows_ref, *refs, ids, pieces, after, assemble, direct, target, stride, all_occ):
    coeff_refs, refs = refs[: max(assemble, 1)], refs[max(assemble, 1) + after :]
    outs, refs = refs[: len(pieces) + bool(assemble)], refs[len(pieces) + bool(assemble) :]
    coeff_all, outs = (outs[0], outs[1:]) if assemble else (None, outs)
    lists, rows, padded, expand, tile_buf, quarter, acc, coeff, tile_sems, sems, *rest = refs
    kl = tile_buf.shape[-1]
    lists_in = pltpu.make_async_copy(lists_ref, lists, sems.at[0])
    lists_in.start()
    rows_in = pltpu.make_async_copy(rows_ref, rows, sems.at[1])
    rows_in.start()
    if assemble:
        *blocks, stacked = rest[: assemble + 1]
        rest = rest[assemble + 1 :]
        coeff_in = [pltpu.make_async_copy(ref, block, sems.at[2 + r]) for r, (ref, block) in enumerate(zip(coeff_refs, blocks))]
        coeff_out = pltpu.make_async_copy(coeff, coeff_all, sems.at[2])
    else:
        coeff_in = [pltpu.make_async_copy(coeff_refs[0], coeff, sems.at[2])]
    for one in coeff_in:
        one.start()
    acc[...] = jnp.zeros_like(acc)
    base = target * 3 * stride
    lists_in.wait()
    groups = (lists[3 * SPREAD * stride + target] + GROUP - 1) // GROUP
    copy = tile_copies(tiles_ref, lists, base, tile_buf, tile_sems)
    for c in range(BUFFERS - 1):
        start_tiles(copy, c, groups)
    rows_in.wait()
    expand_rows(rows, padded, expand)
    for one in coeff_in:
        one.wait()
    if assemble:
        gather_coefficients(blocks, stacked, coeff, rows.shape[0])
        coeff_out.start()
    mask = diagonal_mask()

    def take(c):
        start_tiles(copy, c + BUFFERS - 1, groups)
        for q in range(GROUP):
            copy(c, q).wait()

    def make_quarter(c):
        for q in range(GROUP):
            quarter_tile(mask, expand, lists[base + stride + c * GROUP + q], tile_buf[c % BUFFERS, q], q, ids, quarter)

    def add_group(c):
        left = coeff_group(coeff, lists, base + 2 * stride + c * GROUP, all_occ)
        acc[...] += jnp.dot(left, quarter[...], preferred_element_type=jnp.float32)

    @pl.when(groups > 0)
    def _():
        take(0)
        make_quarter(0)

    def one_group(c, carry):
        take(c + 1)
        add_group(c)
        make_quarter(c + 1)
        return carry

    lax.fori_loop(0, groups - 1, one_group, 0)

    puts = []
    at = 0
    for out, piece in zip(outs, pieces):
        for k in range(piece):
            source = acc.at[:, (at + k) * kl : (at + k + 1) * kl] if direct else rest[0].at[at + k]
            puts.append(pltpu.make_async_copy(source, out.at[k], rest[-1].at[at + k]))
        at += piece

    def finish(total):
        at = 0
        for piece in pieces:
            value = total(slice(at * kl, (at + piece) * kl))
            for k in range(piece):
                if direct:
                    acc[:, (at + k) * kl : (at + k + 1) * kl] = value[:, k * kl : (k + 1) * kl]
                else:
                    rest[0][at + k] = value[:, k * kl : (k + 1) * kl].astype(rest[0].dtype)
                puts[at + k].start()
            at += piece

    @pl.when(groups > 0)
    def _():
        left = coeff_group(coeff, lists, base + 2 * stride + (groups - 1) * GROUP, all_occ)
        finish(lambda cols: acc[:, cols] + jnp.dot(left, quarter[:, cols], preferred_element_type=jnp.float32))

    @pl.when(groups == 0)
    def _():
        finish(lambda cols: acc[:, cols])

    for put in puts:
        put.wait()
    if assemble:
        coeff_out.wait()


def cost(flops, moved):
    return pl.CostEstimate(flops=flops, bytes_accessed=moved, transcendentals=0)


def lists_of(mu_blocks, nu_blocks, tile_live, batch_target, batch_count, stride, nbf):
    return pl.pallas_call(
        functools.partial(list_kernel, stride=stride, zero_block=nbf // NU),
        out_shape=jax.ShapeDtypeStruct((3 * SPREAD * stride + SPREAD,), jnp.int32),
        in_specs=[SMEM] * 5,
        out_specs=SMEM,
        cost_estimate=cost(2_000_000_000, 10_000),
        name="lists",
    )(mu_blocks, nu_blocks, tile_live, batch_target, batch_count)


def partial_sum(lists, tiles, rows, coeff, all_occ, spans, target, stride, dtype, after=()):
    occ, nbf = rows.shape
    kl = tiles.shape[3]
    ids = [i for low, high in spans for i in range(low, high)]
    pieces = [high - low for low, high in spans]
    assemble = len(coeff) if isinstance(coeff, list) else 0
    direct = dtype == jnp.float32
    shapes = [jax.ShapeDtypeStruct((piece, all_occ, kl), dtype) for piece in pieces]
    scratch = [
        pltpu.SMEM(lists.shape, jnp.int32),
        pltpu.VMEM((occ, nbf), BF16),
        pltpu.VMEM((32, nbf), BF16),
        pltpu.VMEM((nbf // 8, 32, 128), jnp.float32),
        pltpu.VMEM((BUFFERS, GROUP, *tiles.shape[1:]), BF16),
        pltpu.VMEM((GROUP * NU, len(ids) * kl), BF16),
        pltpu.VMEM((all_occ, len(ids) * kl), jnp.float32),
        pltpu.VMEM((nbf + NU, 256), BF16),
        pltpu.SemaphoreType.DMA((BUFFERS, GROUP)),
        pltpu.SemaphoreType.DMA((2 + max(assemble, 1),)),
    ]
    if assemble:
        shapes = [jax.ShapeDtypeStruct((nbf + NU, 256), BF16)] + shapes
        scratch += [pltpu.VMEM(block.shape, BF16) for block in coeff] + [pltpu.VMEM((256, nbf), BF16)]
    if not direct:
        scratch += [pltpu.VMEM((len(ids), all_occ, kl), dtype)]
    scratch += [pltpu.SemaphoreType.DMA((len(ids),))]
    coeff = coeff if assemble else [coeff]
    return pl.pallas_call(
        functools.partial(
            partial_kernel, ids=ids, pieces=pieces, after=len(after), assemble=assemble, direct=direct, target=target, stride=stride, all_occ=all_occ
        ),
        out_shape=tuple(shapes),
        in_specs=[ANY] * (3 + len(coeff) + len(after)),
        out_specs=(ANY,) * len(shapes),
        scratch_shapes=scratch,
        compiler_params=pltpu.CompilerParams(vmem_limit_bytes=VMEM_BYTES if direct else None),
        cost_estimate=cost(6_000_000_000, 10_000_000),
        name="partial",
    )(lists, tiles, rows, *coeff, *after)


def local(ao_tiles, mo_coeffs, mu_blocks, nu_blocks, tile_live, batch_target, batch_count):
    nbf, occ = mo_coeffs.shape
    ranks = lax.axis_size("occ")
    tasks = lax.axis_size("task")
    all_occ = occ * ranks
    stride = ao_tiles.shape[0] + GROUP
    rows = mo_coeffs.T

    others = [lax.ppermute(rows, "occ", [((r + 2 * d) % ranks, r) for r in range(ranks)]) for d in range(1, ranks // 2)]
    lists = lists_of(mu_blocks, nu_blocks, tile_live, batch_target, batch_count, stride, nbf)
    others, lists = lax.optimization_barrier((others, lists))
    blocks = []
    for block in [rows] + others:
        blocks += [block, lax.ppermute(block, "occ", [(r ^ 1, r) for r in range(ranks)])]

    ring = 4
    ahead = [(t, (t + 1) % tasks) for t in range(tasks)]
    back = [(t, t // ring * ring + (t - 1) % ring) for t in range(tasks)]
    back_on = [(t // ring * ring + (t - 1) % ring, (t + 2) % tasks) for t in range(tasks)]
    wide = jnp.float32
    cut, half = 8, 19

    def part(**kwargs):
        return partial_sum(lists, ao_tiles, rows, all_occ=all_occ, stride=stride, **kwargs)

    def sent(array, route):
        return lax.ppermute(array, "task", route)

    coeff_all, two_low, two_a, two_b = part(coeff=blocks, spans=[(0, cut), (cut, half), (half, occ)], target=2, dtype=BF16)
    back_a = sent(two_a, back)
    chain = sent(two_low, ahead)
    back_b = sent(two_b, back)
    one_low, one_high = part(coeff=coeff_all, spans=[(0, cut), (cut, occ)], target=1, dtype=BF16)
    near = sent(one_high, ahead)
    far_a = sent(back_a, back_on)
    summed = (chain.astype(wide) + one_low.astype(wide)).astype(BF16)
    last = sent(summed, ahead)
    far_b = sent(back_b, back_on)
    (out,) = part(coeff=coeff_all, spans=[(0, occ)], target=0, dtype=wide, after=(back_b,))
    added = jnp.concatenate([last.astype(wide), near[: half - cut].astype(wide) + far_a.astype(wide), near[half - cut :].astype(wide) + far_b.astype(wide)])
    return out + added


def solution(mesh):
    in_specs = (P("task", None, None, None), P(None, "occ"), P("task"), P("task"), P("task"), P("task"), P("task"))
    return jax.shard_map(local, mesh=mesh, in_specs=in_specs, out_specs=P("occ", None, "task"), check_vma=False)
```
